32 devices in a mesh: gx: 4 (over z), gy: 8 (over y, x, core).
Axes of the slice: x: 2, y: 2, z: 4, core: 2. Of those that a mesh axis runs over, the one named last changes fastest.
Arguments:
- group_one: bfloat16 [6144, 768], P(('gx', 'gy')), may hold values from -6 to 6
- routes_one: int32 [6144, 1], P(('gx', 'gy')), may hold values from 0 to 31; in each aligned block of 192 rows (0 to 191, 192 to 383, ...) at most 6 rows name the same one
- gates_one: float32 [6144], P(('gx', 'gy')), may hold values from 0.2 to 1
- group_two: bfloat16 [6144, 768], P(('gx', 'gy')), may hold values from -6 to 6
- routes_two: int32 [6144, 1], P(('gx', 'gy')), may hold values from 0 to 31; in each aligned block of 192 rows (0 to 191, 192 to 383, ...) at most 6 rows name the same one
- gates_two: float32 [6144], P(('gx', 'gy')), may hold values from 0.2 to 1
- norm_gain: float32 [768], replicated, may hold values from 0.1 to 1.9
- weight_in: bfloat16 [32, 768, 3072], P(('gx', 'gy')), may hold values from -0.21875 to 0.21875
- weight_out: bfloat16 [32, 3072, 768], P(('gx', 'gy')), may hold values from -0.109375 to 0.109375
- old_place: int32 [32], replicated, may hold values from 0 to 31, each once
- partner: int32 [32], replicated, may hold values from 0 to 31, as said below
Outputs:
- result_one: bfloat16 [6144, 768], P(('gx', 'gy'))
- result_two: bfloat16 [6144, 768], P(('gx', 'gy'))
- new_in: bfloat16 [32, 768, 3072], P(('gx', 'gy'))
- new_out: bfloat16 [32, 3072, 768], P(('gx', 'gy'))
The draws below stay inside these ranges and needn't reach their ends.
Inputs may be any that keep to these rules, and one draw needn't show every extreme that they name: `routes_one`: at most 6 tokens of one device's rows in a block name the same expert, a bound that some block reaches of some device's rows in every draw. `routes_two`: same law as routes_one. partner is an involution: partner[partner[s]] = s; exactly 16 slots have partner[s] != s.
All inputs are finite; a program needn't handle non-finite values.
Results may differ from the reference program's by a relative error of at most 0.0041.
Values may be sent and summed in bfloat16 or wider, within the bound.
A program may use at most 128 MiB of HBM per device.

```python
import math
import jax
import jax.numpy as jnp
import numpy as np
from jax import lax

D = 768
FF = 3072
TOK_DEV = 192
CAP = 6
EXPERTS = 32
TOKENS = 6144
EXPERT_ROWS = 192


def draw_partner(key, part):
    shuffled = jax.random.permutation(jax.random.fold_in(key, 7), EXPERTS).astype(jnp.int32)
    moved = EXPERTS // 2
    givers = shuffled[0:moved:2]
    takers = shuffled[1:moved:2]
    labels = jnp.arange(EXPERTS, dtype=jnp.int32)
    return labels.at[givers].set(takers).at[takers].set(givers)


def steps_of(stream_key, extent, split, low, top_value):
    factor_of, own = 1.0, jax.random.fold_in(stream_key, 6)
    for dim, blocks in split:
        heights = jnp.exp(jax.random.uniform(jax.random.fold_in(own, dim), (blocks,), jnp.float32, low / len(split), top_value / len(split)))
        factor_of = factor_of * jnp.repeat(heights, extent[dim] // blocks).reshape([-1 if axis == dim else 1 for axis in range(len(extent))])
    return factor_of


def shared_out(own_key, own, number, rows, count, top, limit, slope):
    sequence = jax.random.permutation(own_key, count)
    heavy_load, common = portions_of(count, rows * top, limit, slope, True), portions_of(count, rows * top, limit, slope, False)
    places = jnp.arange(count)

    def named(lengths, offset_by):
        used = int((lengths > 0).sum())
        fixed = max(1, used // 4)
        shifted = fixed + (places - fixed + offset_by * (used - fixed)) % max(1, count - fixed)
        return jnp.zeros((count,), jnp.int32).at[sequence[jnp.where(places < fixed, places, shifted)]].set(jnp.asarray(lengths, jnp.int32))

    lengths = jnp.where(number % 4 == 0, named(heavy_load, number // 4), named(common, number - number // 4 - 1))
    mixed = jax.random.permutation(jax.random.fold_in(own, 3), count)
    giver, taker = mixed[0:count // 2 * 2:2], mixed[1:count // 2 * 2:2]
    margin = jnp.minimum(lengths[giver] - 1, limit - lengths[taker]) // 2
    margin = jnp.where((giver == sequence[0]) | (taker == sequence[0]) | (lengths[taker] == 0), 0, jnp.maximum(margin, 0))
    shifted = jax.random.randint(jax.random.fold_in(own, 4), (count // 2,), 0, 1 << 20) % (margin + 1)
    lengths = lengths.at[giver].add(-shifted).at[taker].add(shifted)
    items = jnp.searchsorted(jnp.cumsum(lengths), jnp.arange(rows * top), side="right").astype(jnp.int32)
    table = items.reshape(top, rows).T
    table = table[jax.random.permutation(jax.random.fold_in(own, 1), rows)]
    offset_by = jax.random.randint(jax.random.fold_in(own, 2), (rows, 1), 0, top)
    return jnp.take_along_axis(table, (jnp.arange(top)[None, :] + offset_by) % top, axis=1)


def portions_of(number_of, total, bound, lean, full):
    weights = [(1 << 20) // math.isqrt(grade ** lean) + 1 for grade in range(1, number_of + 1)]
    largest = bound if full else min(bound, max(-(-total // number_of), total * weights[0] // sum(weights)))
    least = 1 if total - largest >= number_of - 1 else 0
    given, spare = [largest] + [least] * (number_of - 1), total - largest - least * (number_of - 1)
    while spare > 0:
        free = [i for i in range(1, number_of) if given[i] < largest] or [i for i in range(1, number_of) if given[i] < bound]
        whole, remaining = sum([weights[i] for i in free]), spare
        for i in free:
            extra = min(bound - given[i], max(1, remaining * weights[i] // whole), spare)
            given[i] = given[i] + extra
            spare = spare - extra
    return np.array(given)


def centred(rng, extent, width, most, cuts=(), kind=jnp.bfloat16):
    drawn = width * jax.random.normal(rng, extent, jnp.float32)
    if cuts:
        drawn = drawn * steps_of(rng, extent, cuts, -0.22, 0.18)
    return jnp.clip(drawn, -most, most).astype(kind)


def setup_inputs(seed: int = 0) -> dict:
    arg_keys = jax.random.split(jax.random.key(seed), 12)
    group_one = centred(arg_keys[0], (TOKENS, D), 1.0, 6.0, ((0, 32),))
    routes_one_keys = jax.random.split(jax.random.fold_in(arg_keys[1], 1), TOKENS // TOK_DEV)
    routes_one_turns = jax.random.permutation(jax.random.fold_in(arg_keys[1], 3), TOKENS // TOK_DEV)
    routes_one = jax.vmap(lambda own, number: shared_out(jax.random.fold_in(arg_keys[1], 2), own, number, TOK_DEV, EXPERTS, 1, CAP, 2))(routes_one_keys, routes_one_turns).reshape((TOKENS, 1))
    gates_one = jnp.clip(0.2 + 0.8 * jax.random.uniform(arg_keys[2], (TOKENS,), jnp.float32) ** steps_of(arg_keys[2], (TOKENS,), ((0, 32),), -0.2, 0.2), 0.2, 1.0)
    group_two = centred(arg_keys[3], (TOKENS, D), 1.0, 6.0, ((0, 32),))
    routes_two_keys = jax.random.split(jax.random.fold_in(arg_keys[4], 1), TOKENS // TOK_DEV)
    routes_two_turns = jax.random.permutation(jax.random.fold_in(arg_keys[4], 3), TOKENS // TOK_DEV)
    routes_two = jax.vmap(lambda own, number: shared_out(jax.random.fold_in(arg_keys[4], 2), own, number, TOK_DEV, EXPERTS, 1, CAP, 2))(routes_two_keys, routes_two_turns).reshape((TOKENS, 1))
    gates_two = jnp.clip(0.2 + 0.8 * jax.random.uniform(arg_keys[5], (TOKENS,), jnp.float32) ** steps_of(arg_keys[5], (TOKENS,), ((0, 32),), -0.2, 0.2), 0.2, 1.0)
    norm_gain = jnp.clip(1.0 + 0.18 * jax.random.normal(arg_keys[6], (D,), jnp.float32), 0.1, 1.9)
    weight_in = centred(arg_keys[7], (EXPERTS, D, FF), D ** -0.5, 0.21875, ((0, 32),))
    weight_out = centred(arg_keys[8], (EXPERTS, FF, D), FF ** -0.5, 0.109375, ((0, 32),))
    old_place = jax.random.permutation(arg_keys[9], EXPERTS).astype(jnp.int32)
    partner = draw_partner(jax.random.fold_in(arg_keys[11], 71), 0)
    return {"group_one": group_one, "routes_one": routes_one, "gates_one": gates_one, "group_two": group_two, "routes_two": routes_two, "gates_two": gates_two, "norm_gain": norm_gain, "weight_in": weight_in, "weight_out": weight_out, "old_place": old_place, "partner": partner}


epsilon = 1e-06

def expert_table(routes):
    expert_ids = routes[:, 0].astype(jnp.int32)
    ordering = jnp.argsort(expert_ids, stable=True).astype(jnp.int32)
    sorted_ids = expert_ids[ordering]
    counts = jnp.zeros((EXPERTS,), jnp.int32).at[expert_ids].add(1)
    starts = jnp.cumsum(counts).astype(jnp.int32) - counts
    placed = jnp.arange(TOKENS, dtype=jnp.int32) - starts[sorted_ids]
    row_table = jnp.full((EXPERTS, EXPERT_ROWS), TOKENS, jnp.int32)
    return row_table.at[sorted_ids, placed].set(ordering)

def switch_layer(tokens_in, routes, gate_probs, norm_gain, weight_in, weight_out, holder):
    values = tokens_in.astype(jnp.float32)
    scaling = lax.rsqrt(lax.optimization_barrier(jnp.mean(values * values, axis=1, keepdims=True)) + epsilon)
    normed = (values * scaling * norm_gain.astype(jnp.float32)).astype(jnp.bfloat16)
    padded = jnp.concatenate([normed, jnp.zeros((1, D), jnp.bfloat16)], axis=0)
    row_table = expert_table(routes)

    def one_expert(members):
        entries, holder_slot = members
        inputs = padded[entries]
        hidden = jnp.maximum(jnp.dot(inputs, weight_in[holder_slot], preferred_element_type=jnp.float32), 0.0).astype(jnp.bfloat16)
        return jnp.dot(hidden, weight_out[holder_slot], preferred_element_type=jnp.float32).astype(jnp.bfloat16)
    outputs = lax.map(one_expert, (row_table, holder))
    gathered = jnp.zeros((TOKENS + 1, D), jnp.bfloat16).at[row_table].set(outputs)[:TOKENS]
    mixed = values + gate_probs.astype(jnp.float32)[:, None] * gathered.astype(jnp.float32)
    return mixed.astype(jnp.bfloat16)

def reference(group_one, routes_one, gates_one, group_two, routes_two, gates_two, norm_gain, weight_in, weight_out, old_place, partner):
    holder = jnp.argsort(old_place).astype(jnp.int32)
    first_out = switch_layer(group_one, routes_one, gates_one, norm_gain, weight_in, weight_out, holder)
    second = switch_layer(group_two, routes_two, gates_two, norm_gain, weight_in, weight_out, holder)
    new_in = jnp.take(weight_in, partner, axis=0)
    new_out = jnp.take(weight_out, partner, axis=0)
    return (first_out, second, new_in, new_out)
```

```python
import jax
import jax.numpy as jnp
from jax import lax
from jax.experimental import pallas as pl
from jax.experimental.pallas import tpu as pltpu
from jax.sharding import PartitionSpec as P

CAP = 6
PARTS_IN = 2
PARTS_OUT = 2
AXES = ("gx", "gy")

epsilon = 1e-06


def pick_kernel(count, sel, idx, *refs):
    del idx
    out = refs[count]
    here = sel[pl.program_id(0)]
    for j in range(count):
        def put(j=j):
            out[...] = refs[j][...]
        pl.when(here == j)(put)


def pick(sources, sel, idx):
    total, rows, columns = sources[0].shape
    block = (1, rows, columns)

    def source_spec(j):
        return pl.BlockSpec(
            block, lambda i, sel, idx: (jnp.where(sel[i] == j, idx[i], 0), 0, 0)
        )

    size = total * rows * columns
    return pl.pallas_call(
        lambda *refs: pick_kernel(len(sources), *refs),
        out_shape=jax.ShapeDtypeStruct(sources[0].shape, sources[0].dtype),
        grid_spec=pltpu.PrefetchScalarGridSpec(
            num_scalar_prefetch=2,
            grid=(total,),
            in_specs=[source_spec(j) for j in range(len(sources))],
            out_specs=pl.BlockSpec(block, lambda i, sel, idx: (i, 0, 0)),
        ),
        cost_estimate=pl.CostEstimate(
            flops=size * 256, bytes_accessed=size * 4, transcendentals=0
        ),
        name="pick",
    )(sel, idx, *sources)


def rows_of(table, keys):
    labels = lax.iota(jnp.int32, table.shape[0])
    return jnp.sum(jnp.where(keys[:, None] == labels[None, :], table[None, :], 0), axis=1)


def routing(partner):
    planes, width = lax.axis_size("gx"), lax.axis_size("gy")
    slots = planes * width
    here = lax.axis_index("gx")
    half_size = slots // 2
    labels = lax.iota(jnp.int32, slots)
    half_of = labels // half_size
    crossing = (partner // half_size) != half_of
    earlier = (labels[None, :] < labels[:, None]) & (half_of[None, :] == half_of[:, None])
    rank = jnp.sum(jnp.where(earlier & crossing[None, :], 1, 0), axis=1)
    mine = crossing & (half_of == (here * width) // half_size)
    order = lax.iota(jnp.int32, width)
    wanted = mine[None, :] & (rank[None, :] == order[:, None])
    leaving = jnp.sum(jnp.where(wanted, labels[None, :], 0), axis=1)
    mid = (jnp.where(leaving // width == here, 0, 1), leaving % width)

    def into(plane):
        source = lax.dynamic_slice(partner, (plane * width,), (width,))
        near = (source // half_size) == (here * width) // half_size
        sel = jnp.where(near, jnp.where(source // width == here, 0, 1), 2)
        return sel, jnp.where(near, source % width, rows_of(rank, source))

    sel, idx = into(here)
    middle = (here == 1) | (here == 2)
    last = (jnp.where(middle, sel, 3), jnp.where(middle, idx, order))
    return mid, into(jnp.bitwise_xor(here, 1)), last


def relocate_part(piece, tables):
    mid, outward, last = tables
    own = lax.all_to_all(piece, "gy", split_axis=0, concat_axis=0, tiled=True)
    outer = lax.ppermute(own, "gx", [(0, 1), (3, 2)])
    leaving = pick((own, outer), *mid)
    across = lax.ppermute(leaving, "gx", [(1, 2), (2, 1)])
    returning = pick((own, outer, across), *outward)
    back = lax.ppermute(returning, "gx", [(1, 0), (2, 3)])
    settled = pick((own, outer, across, back), *last)
    return lax.all_to_all(settled, "gy", split_axis=0, concat_axis=0, tiled=True)


def relocate_by_planes(weight_in, weight_out, partner):
    width = lax.axis_size("gy")
    tables = routing(partner)
    results = []
    for weight, parts in ((weight_in, PARTS_IN), (weight_out, PARTS_OUT)):
        _, rows, columns = weight.shape
        chunk = rows // parts
        done = []
        for part in range(parts):
            piece = weight[0, part * chunk : (part + 1) * chunk]
            piece = piece.reshape(width, chunk // width, columns)
            done.append(relocate_part(piece, tables).reshape(chunk, columns))
        results.append(jnp.concatenate(done, axis=0)[None])
    return tuple(results)


def relocate_flat(weight_in, weight_out, partner):
    devices = lax.axis_size(AXES)
    stacked = jnp.stack([weight_in.reshape(devices, -1), weight_out.reshape(devices, -1)], axis=1)
    pieces = lax.all_to_all(stacked, AXES, split_axis=0, concat_axis=0, tiled=True)
    reordered = jnp.take(pieces, partner, axis=0)
    settled = lax.all_to_all(reordered, AXES, split_axis=0, concat_axis=0, tiled=True)
    return (settled[:, 0].reshape(weight_in.shape), settled[:, 1].reshape(weight_out.shape))


def both_blocks(groups, routes, gates, norm_gain, old_place, weight_in, weight_out):
    devices = lax.axis_size(AXES)
    rows, model_width = groups[0].shape
    slots = lax.iota(jnp.int32, devices)
    places = []
    lower = (
        lax.broadcasted_iota(jnp.int32, (rows, rows), 0)
        > lax.broadcasted_iota(jnp.int32, (rows, rows), 1)
    ).astype(jnp.bfloat16)
    for block, names in enumerate(routes):
        member = names == old_place[None, :]
        before = jnp.dot(lower, member.astype(jnp.bfloat16), preferred_element_type=jnp.float32)
        spot = slots[None, :] * (2 * CAP) + block * CAP + before.astype(jnp.int32)
        places.append(jnp.sum(jnp.where(member, spot, 0), axis=1))
    place = jnp.concatenate(places)
    total = devices * 2 * CAP
    values = jnp.concatenate(groups, axis=0).astype(jnp.float32)
    scaling = lax.rsqrt(jnp.mean(values * values, axis=1, keepdims=True) + epsilon)
    normed = (values * scaling * norm_gain).astype(jnp.bfloat16)
    chosen = (lax.iota(jnp.int32, total)[:, None] == place[None, :]).astype(jnp.bfloat16)
    outgoing = jnp.dot(chosen, normed, preferred_element_type=jnp.float32).astype(jnp.bfloat16)
    arrived = lax.all_to_all(
        outgoing.reshape(devices, 2 * CAP, model_width), AXES, split_axis=0, concat_axis=0, tiled=True
    ).reshape(total, model_width)
    hidden = jnp.maximum(
        jnp.dot(arrived, weight_in[0], preferred_element_type=jnp.float32), 0.0
    ).astype(jnp.bfloat16)
    result = jnp.dot(hidden, weight_out[0], preferred_element_type=jnp.float32).astype(jnp.bfloat16)
    returned = lax.all_to_all(
        result.reshape(devices, 2 * CAP, model_width), AXES, split_axis=0, concat_axis=0, tiled=True
    ).reshape(total, model_width)
    answer = lax.dot_general(
        chosen, returned, (((0,), (0,)), ((), ())), preferred_element_type=jnp.float32
    )
    gate = jnp.concatenate(gates)[:, None]
    mixed = (values + gate * answer).astype(jnp.bfloat16)
    return mixed[:rows], mixed[rows:]


def local(
    group_one,
    routes_one,
    gates_one,
    group_two,
    routes_two,
    gates_two,
    norm_gain,
    weight_in,
    weight_out,
    old_place,
    partner,
):
    first, second = both_blocks(
        (group_one, group_two),
        (routes_one, routes_two),
        (gates_one, gates_two),
        norm_gain,
        old_place,
        weight_in,
        weight_out,
    )
    relocate = relocate_by_planes if lax.axis_size("gx") == 4 else relocate_flat
    new_in, new_out = relocate(weight_in, weight_out, partner)
    return (first, second, new_in, new_out)


def solution(mesh):
    split = ("gx", "gy")
    rows, flat, cube = P(split, None), P(split), P(split, None, None)
    return jax.shard_map(
        local,
        mesh=mesh,
        in_specs=(rows, rows, flat, rows, rows, flat, P(), cube, cube, P(), P()),
        out_specs=(rows, rows, cube, cube),
        check_vma=False,
    )
```

```python
import functools

import jax
import jax.numpy as jnp
from jax import lax
from jax.experimental import pallas as pl
from jax.experimental.pallas import tpu as pltpu
from jax.sharding import PartitionSpec as P

CAP = 6
PARTS_IN = 2
PARTS_OUT = 2
ROOMS = (5, 6)
AXES = ("gx", "gy")

epsilon = 1e-06


def pick_kernel(count, sel, idx, *refs):
    del idx
    out = refs[count]
    here = sel[pl.program_id(0)]
    for j in range(count):
        def put(j=j):
            out[...] = refs[j][...]
        pl.when(here == j)(put)


def pick(sources, sel, idx):
    total = sel.shape[0]
    _, rows, columns = sources[0].shape
    block = (1, rows, columns)

    def source_spec(j):
        end = sources[j].shape[0] - 1
        return pl.BlockSpec(
            block,
            lambda i, sel, idx: (jnp.where(sel[i] == j, jnp.minimum(idx[i], end), 0), 0, 0),
        )

    size = total * rows * columns
    return pl.pallas_call(
        lambda *refs: pick_kernel(len(sources), *refs),
        out_shape=jax.ShapeDtypeStruct((total, rows, columns), sources[0].dtype),
        grid_spec=pltpu.PrefetchScalarGridSpec(
            num_scalar_prefetch=2,
            grid=(total,),
            in_specs=[source_spec(j) for j in range(len(sources))],
            out_specs=pl.BlockSpec(block, lambda i, sel, idx: (i, 0, 0)),
        ),
        cost_estimate=pl.CostEstimate(
            flops=size * 256, bytes_accessed=size * 4, transcendentals=0
        ),
        name="pick",
    )(sel, idx, *sources)


def rows_of(table, keys):
    labels = lax.iota(jnp.int32, table.shape[0])
    return jnp.sum(jnp.where(keys[:, None] == labels[None, :], table[None, :], 0), axis=1)


def ranks(partner):
    width = lax.axis_size("gy")
    slots = lax.axis_size("gx") * width
    labels = lax.iota(jnp.int32, slots)
    half_size = slots // 2
    moved = partner != labels
    crossing = (partner // half_size) != (labels // half_size)
    earlier = labels[None, :] < labels[:, None]

    def rank(chosen, group):
        same = group[None, :] == group[:, None]
        return jnp.sum(jnp.where(earlier & same & chosen[None, :], 1, 0), axis=1)

    return moved, crossing, rank(moved, labels // width), rank(crossing, labels // half_size)


def needed(partner):
    planes, width = lax.axis_size("gx"), lax.axis_size("gy")
    labels = lax.iota(jnp.int32, planes * width)
    moved, crossing, _, _ = ranks(partner)
    plane = labels // width
    first = jnp.sum(jnp.where(moved & (plane == 0), 1, 0))
    last = jnp.sum(jnp.where(moved & (plane == planes - 1), 1, 0))
    across = jnp.sum(jnp.where(crossing & (plane < planes // 2), 1, 0))
    return jnp.maximum(jnp.maximum(first, last), across)


def routing(partner, room):
    planes, width = lax.axis_size("gx"), lax.axis_size("gy")
    here = lax.axis_index("gx")
    half_size = planes * width // 2
    labels = lax.iota(jnp.int32, planes * width)
    moved, crossing, spot, rank = ranks(partner)
    order = lax.iota(jnp.int32, room)
    whole = lax.iota(jnp.int32, width)

    def listed(chosen, position):
        wanted = chosen[None, :] & (position[None, :] == order[:, None])
        return jnp.sum(jnp.where(wanted, labels[None, :], 0), axis=1)

    def place(source):
        near = (source // half_size) == (here * width) // half_size
        own = source // width == here
        sel = jnp.where(near, jnp.where(own, 0, 1), 2)
        inner = jnp.where(own, source % width, rows_of(spot, source))
        return sel, jnp.where(near, inner, rows_of(rank, source))

    outgoing = listed(moved & (labels // width == here), spot) % width
    inward = (jnp.zeros_like(outgoing), outgoing)
    mine = crossing & (labels // half_size == (here * width) // half_size)
    leaving = listed(mine, rank)
    mid = (
        jnp.where(leaving // width == here, 0, 1),
        jnp.where(leaving // width == here, leaving % width, rows_of(spot, leaving)),
    )
    outer = jnp.bitwise_xor(here, 1)
    targets = listed(moved & (labels // width == outer), spot)
    outward = place(rows_of(partner, targets))
    sel, idx = place(lax.dynamic_slice(partner, (here * width,), (width,)))
    stays = jnp.logical_not(lax.dynamic_slice(moved, (here * width,), (width,)))
    own_spot = lax.dynamic_slice(spot, (here * width,), (width,))
    middle = (here == 1) | (here == 2)
    last = (
        jnp.where(stays, 0, jnp.where(middle, sel, 3)),
        jnp.where(stays, whole, jnp.where(middle, idx, own_spot)),
    )
    return inward, mid, outward, last


def spread(piece):
    return lax.all_to_all(piece, "gy", split_axis=0, concat_axis=0, tiled=True)


def relocate_part(own, tables):
    inward, mid, outward, last = tables
    outer = lax.ppermute(pick((own,), *inward), "gx", [(0, 1), (3, 2)])
    across = lax.ppermute(pick((own, outer), *mid), "gx", [(1, 2), (2, 1)])
    returning = pick((own, outer, across), *outward)
    back = lax.ppermute(returning, "gx", [(1, 0), (2, 3)])
    return spread(pick((own, outer, across, back), *last))


def by_planes(room, tokens, weight_in, weight_out, old_place, partner):
    width = lax.axis_size("gy")
    pieces = []
    for weight, parts in ((weight_in, PARTS_IN), (weight_out, PARTS_OUT)):
        _, rows, columns = weight.shape
        chunk = rows // parts
        for part in range(parts):
            piece = weight[0, part * chunk : (part + 1) * chunk]
            pieces.append(piece.reshape(width, chunk // width, columns))
    first = spread(pieces[0])
    first, tokens = lax.optimization_barrier((first, tokens))
    results = both_blocks(*tokens, old_place, weight_in, weight_out)
    tables = routing(partner, room)
    done = [relocate_part(first, tables)]
    done += [relocate_part(spread(piece), tables) for piece in pieces[1:]]
    new_in = jnp.concatenate(done[:PARTS_IN], axis=0).reshape(weight_in.shape)
    new_out = jnp.concatenate(done[PARTS_IN:], axis=0).reshape(weight_out.shape)
    return (*results, new_in, new_out)


def relocate_flat(weight_in, weight_out, partner):
    devices = lax.axis_size(AXES)
    stacked = jnp.stack([weight_in.reshape(devices, -1), weight_out.reshape(devices, -1)], axis=1)
    pieces = lax.all_to_all(stacked, AXES, split_axis=0, concat_axis=0, tiled=True)
    reordered = jnp.take(pieces, partner, axis=0)
    settled = lax.all_to_all(reordered, AXES, split_axis=0, concat_axis=0, tiled=True)
    return (settled[:, 0].reshape(weight_in.shape), settled[:, 1].reshape(weight_out.shape))


def both_blocks(groups, routes, gates, norm_gain, old_place, weight_in, weight_out):
    devices = lax.axis_size(AXES)
    rows, model_width = groups[0].shape
    slots = lax.iota(jnp.int32, devices)
    places = []
    lower = (
        lax.broadcasted_iota(jnp.int32, (rows, rows), 0)
        > lax.broadcasted_iota(jnp.int32, (rows, rows), 1)
    ).astype(jnp.bfloat16)
    for block, names in enumerate(routes):
        member = names == old_place[None, :]
        before = jnp.dot(lower, member.astype(jnp.bfloat16), preferred_element_type=jnp.float32)
        spot = slots[None, :] * (2 * CAP) + block * CAP + before.astype(jnp.int32)
        places.append(jnp.sum(jnp.where(member, spot, 0), axis=1))
    place = jnp.concatenate(places)
    total = devices * 2 * CAP
    values = jnp.concatenate(groups, axis=0).astype(jnp.float32)
    scaling = lax.rsqrt(jnp.mean(values * values, axis=1, keepdims=True) + epsilon)
    normed = (values * scaling * norm_gain).astype(jnp.bfloat16)
    chosen = (lax.iota(jnp.int32, total)[:, None] == place[None, :]).astype(jnp.bfloat16)
    outgoing = jnp.dot(chosen, normed, preferred_element_type=jnp.float32).astype(jnp.bfloat16)
    arrived = lax.all_to_all(
        outgoing.reshape(devices, 2 * CAP, model_width), AXES, split_axis=0, concat_axis=0, tiled=True
    ).reshape(total, model_width)
    hidden = jnp.maximum(
        jnp.dot(arrived, weight_in[0], preferred_element_type=jnp.float32), 0.0
    ).astype(jnp.bfloat16)
    result = jnp.dot(hidden, weight_out[0], preferred_element_type=jnp.float32).astype(jnp.bfloat16)
    returned = lax.all_to_all(
        result.reshape(devices, 2 * CAP, model_width), AXES, split_axis=0, concat_axis=0, tiled=True
    ).reshape(total, model_width)
    answer = lax.dot_general(
        chosen, returned, (((0,), (0,)), ((), ())), preferred_element_type=jnp.float32
    )
    gate = jnp.concatenate(gates)[:, None]
    mixed = (values + gate * answer).astype(jnp.bfloat16)
    return mixed[:rows], mixed[rows:]


def local(
    group_one,
    routes_one,
    gates_one,
    group_two,
    routes_two,
    gates_two,
    norm_gain,
    weight_in,
    weight_out,
    old_place,
    partner,
):
    tokens = (
        (group_one, group_two),
        (routes_one, routes_two),
        (gates_one, gates_two),
        norm_gain,
    )
    if lax.axis_size("gx") != 4:
        results = both_blocks(*tokens, old_place, weight_in, weight_out)
        return (*results, *relocate_flat(weight_in, weight_out, partner))
    width = lax.axis_size("gy")
    rooms = sorted({max(1, width * share // 8) for share in ROOMS} | {width})
    need = needed(partner)
    branch = sum((need > room).astype(jnp.int32) for room in rooms[:-1])
    return lax.switch(
        branch,
        [functools.partial(by_planes, room) for room in rooms],
        tokens,
        weight_in,
        weight_out,
        old_place,
        partner,
    )


def solution(mesh):
    split = ("gx", "gy")
    rows, flat, cube = P(split, None), P(split), P(split, None, None)
    return jax.shard_map(
        local,
        mesh=mesh,
        in_specs=(rows, rows, flat, rows, rows, flat, P(), cube, cube, P(), P()),
        out_specs=(rows, rows, cube, cube),
        check_vma=False,
    )
```
